8 devices in a mesh: depth: 2 (over z, y), col: 2 (over x), row: 2 (over core).
Axes of the slice: x: 2, y: 2, z: 1, core: 2. Of those that a mesh axis runs over, the one named last changes fastest.
Arguments:
- reach_in: bfloat16 [5120, 5120], P(('row', 'depth'), 'col')
Outputs:
- output: bfloat16 [5120, 5120], P(('row', 'depth'), 'col')
All inputs are finite; a program needn't handle non-finite values.
Results may differ from the reference program's by a relative error of at most 0.001.
Values are sent between devices in bfloat16 or wider.
A program may use at most 1 GiB of HBM per device.

```python
import jax
import jax.numpy as jnp
from jax import lax

N = 5120
SQUARINGS = 4


def setup_inputs(seed: int = 0) -> dict:
    root_key = jax.random.key(seed)
    position = jax.random.permutation(root_key, N)
    chain_edges = position[None, :] == position[:, None] + 1
    return {'reach_in': chain_edges.astype(jnp.float32).astype(jnp.bfloat16)}


def reference(reach_in):
    def square_once(current, unused_x):
        path_count = jnp.dot(current, current, preferred_element_type=jnp.float32)
        next_reach = jnp.minimum(path_count + current.astype(jnp.float32), 1.0).astype(jnp.bfloat16)
        return next_reach, None
    final_reach, unused_ys = lax.scan(square_once, reach_in, None, length=SQUARINGS)
    return final_reach
```

```python
import functools

import jax
import jax.numpy as jnp
from jax import lax
from jax.experimental import pallas as pl
from jax.experimental.pallas import tpu as pltpu
from jax.sharding import PartitionSpec as P

MESH = pl.DeviceIdType.MESH
NC = 10
SHARE2 = 6
SHARE3 = 5


def kernel(n, s_ref, o_ref, r0, r1, r2, r3, panel, bbuf,
           loc, ps, pr, xs, xr, ys, yr, bsem, osem, rdy):
    half, slab, width = n // 2, n // 4, n // (2 * NC)
    l = lax.axis_index('depth')
    j = lax.axis_index('col')
    i = lax.axis_index('row')
    x_dev, y_dev, p_dev = {'col': 1 - j}, {'depth': 1 - l}, {'row': 1 - i}

    def mo(v, m):
        return pl.multiple_of(v, m)

    def rows(ls):
        return pl.ds(mo(ls * slab, slab), slab)

    def cols(c):
        return pl.ds(mo(c * width, width), width)

    def pv(buf, ls, c):
        return panel.at[buf, rows(ls), cols(c)]

    def rv(r, ls, c):
        return r.at[pl.ds(mo(i * half + ls * slab, slab), slab), cols(c)]

    def remote(src, dst, ssem, rsem, dev):
        return pltpu.make_async_remote_copy(
            src_ref=src, dst_ref=dst, send_sem=ssem, recv_sem=rsem, device_id=dev, device_id_type=MESH)

    def local_copy(k, buf, r, ls, c):
        return pltpu.make_async_copy(pv(buf, ls, c), rv(r, ls, c), loc.at[k, ls * 2 * NC + c])

    def partner_copy(k, src, r, ls, c):
        q = ls * 2 * NC + c
        return remote(src, rv(r, ls, c), ps.at[k, q], pr.at[k, q], p_dev)

    def x_copy(k, src, dst, q):
        return remote(src, dst, xs.at[k, q], xr.at[k, q], x_dev)

    def y_copy(k, src, dst, q):
        return remote(src, dst, ys.at[k, q], yr.at[k, q], y_dev)

    def b_copy(r, c, slot):
        return pltpu.make_async_copy(r.at[:, cols(c)], bbuf.at[slot], bsem.at[slot])

    def compute(src, dst, ls, c, slot):
        acc = jnp.dot(panel[src, rows(ls), :], bbuf[slot], preferred_element_type=jnp.float32)
        old = panel[src, rows(ls), cols(c)].astype(jnp.float32)
        panel[dst, rows(ls), cols(c)] = jnp.minimum(acc + old, 1.0).astype(jnp.bfloat16)

    def for_each(count, body, start=0):
        def step(q, carry):
            body(q)
            return carry
        lax.fori_loop(start, count, step, 0)

    def unit_loop(count, where, r, src, dst, after):
        b_copy(r, where(0)[1], 0).start()

        def body(u):
            slot = lax.rem(u, 2)
            ls, c = where(u)

            @pl.when(u + 1 < count)
            def _():
                b_copy(r, where(u + 1)[1], 1 - slot).start()
            b_copy(r, c, slot).wait()
            compute(src, dst, ls, c, slot)
            after(u, ls, c)
        for_each(count, body)

    mine, other = j * NC, (1 - j) * NC

    barrier = pltpu.get_barrier_semaphore()
    for dev in (x_dev, y_dev, p_dev):
        pl.semaphore_signal(barrier, inc=1, device_id=dev, device_id_type=MESH)
    pl.semaphore_wait(barrier, 3)

    def own(p):
        return s_ref.at[:, cols(p)]

    def start_own(p):
        x_copy(0, own(p), pv(0, l, mine + p), p).start()
        y_copy(0, own(p), pv(0, l, mine + p), p).start()
        partner_copy(0, own(p), r0, l, mine + p).start()
    for_each(NC, start_own)
    own_load = pltpu.make_async_copy(
        s_ref, panel.at[0, rows(l), pl.ds(mo(j * half, half), half)], osem.at[0])
    own_load.start()
    own_load.wait()
    for_each(NC, lambda p: local_copy(0, 0, r0, l, mine + p).start())

    def spread(ls, c):
        local_copy(0, 0, r0, ls, c).start()
        partner_copy(0, pv(0, ls, c), r0, ls, c).start()

    def relay(p):
        x_copy(0, own(p), pv(0, l, other + p), p).wait_recv()
        spread(l, other + p)

        @pl.when(lax.rem(p, 2) == 1)
        def _():
            y_copy(0, pv(0, l, other + p), pv(0, l, other + p), NC + p // 2).start()
        y_copy(0, own(p), pv(0, 1 - l, mine + p), p).wait_recv()
        spread(1 - l, mine + p)

        @pl.when(lax.rem(p, 2) == 0)
        def _():
            x_copy(0, pv(0, 1 - l, mine + p), pv(0, 1 - l, mine + p), NC + p // 2).start()
    for_each(NC, relay)

    def diagonal(q):
        c = other + 2 * q
        x_copy(0, own(0), pv(0, 1 - l, c), NC + q).wait_recv()
        spread(1 - l, c)
        y_copy(0, own(0), pv(0, 1 - l, c + 1), NC + q).wait_recv()
        spread(1 - l, c + 1)
    for_each(NC // 2, diagonal)

    def drain(k, r):
        def body(q):
            for ls in (0, 1):
                local_copy(k, 0, r, ls, q).wait()
                partner_copy(k, pv(0, ls, q), r, ls, q).wait()
        for_each(2 * NC, body)

    def drain_sends(k, count):
        def body(q):
            x_copy(k, own(0), pv(0, 0, 0), q).wait_send()
            y_copy(k, own(0), pv(0, 0, 0), q).wait_send()
        for_each(count, body)

    def ready(k):
        for dev in (x_dev, y_dev):
            pl.semaphore_signal(rdy.at[k], inc=1, device_id=dev, device_id_type=MESH)

    drain(0, r0)
    drain_sends(0, NC + NC // 2)

    def publish(k, buf, r, ls, c):
        local_copy(k, buf, r, ls, c).start()
        partner_copy(k, pv(buf, ls, c), r, ls, c).start()

    unit_loop(4 * NC, lambda u: (lax.rem(u, 2), u // 2), r0, 0, 1,
              lambda u, ls, c: publish(1, 1, r1, ls, c))
    ready(0)
    drain(1, r1)

    def where2(u):
        first = u < NC
        second = u < 2 * NC
        third = u < 3 * NC - SHARE2
        ls = jnp.where(first | (~second & third), l, 1 - l)
        c = jnp.where(first, mine + u, jnp.where(second, other + u - NC, jnp.where(
            third, other + SHARE2 + u - 2 * NC, mine + 2 * SHARE2 + u - 3 * NC)))
        return ls, c

    def receive2(q):
        x_copy(1, own(0), pv(0, l, other + q), q).wait_recv()
        publish(2, 0, r2, l, other + q)
        y_copy(1, own(0), pv(0, 1 - l, mine + q), q).wait_recv()
        publish(2, 0, r2, 1 - l, mine + q)

    units2 = 4 * NC - 2 * SHARE2
    in_loop2 = min(SHARE2, units2 // 4 - 1)

    def after2(u, ls, c):
        publish(2, 0, r2, ls, c)

        @pl.when(u == 0)
        def _():
            pl.semaphore_wait(rdy.at[0], 2)

        @pl.when(u < SHARE2)
        def _():
            x_copy(1, pv(0, l, mine + u), pv(0, l, mine + u), u).start()
            y_copy(1, pv(0, l, mine + u), pv(0, l, mine + u), u).start()

        @pl.when((lax.rem(u, 4) == 3) & (u >= 4) & (u // 4 - 1 < in_loop2))
        def _():
            receive2(u // 4 - 1)

    unit_loop(units2, where2, r1, 1, 0, after2)
    for_each(SHARE2, receive2, start=in_loop2)
    ready(1)
    drain(2, r2)
    drain_sends(1, SHARE2)

    def where3(u):
        first = u < NC
        second = u < 2 * NC - SHARE3
        ls = jnp.where(second, l, 1 - l)
        c = jnp.where(first, mine + u, jnp.where(second, other + SHARE3 + u - NC, mine + 2 * SHARE3 + u - 2 * NC))
        return ls, c

    def receive3(q):
        y_copy(2, own(0), rv(r3, 1 - l, mine + q), q).wait_recv()
        partner_copy(3, rv(r3, 1 - l, mine + q), r3, 1 - l, mine + q).start()

    units3 = 3 * NC - 2 * SHARE3
    in_loop3 = min(SHARE3, units3 // 4 - 1)

    def after3(u, ls, c):
        @pl.when((u < NC) | (u >= 2 * NC - SHARE3))
        def _():
            publish(3, 1, r3, ls, c)

        @pl.when(u == 0)
        def _():
            pl.semaphore_wait(rdy.at[1], 2)

        @pl.when(u < SHARE3)
        def _():
            x_copy(2, pv(1, l, mine + u), pv(1, l, mine + u), u).start()
            y_copy(2, pv(1, l, mine + u), rv(r3, l, mine + u), u).start()

        @pl.when((lax.rem(u, 4) == 3) & (u >= 4) & (u // 4 - 1 < in_loop3))
        def _():
            receive3(u // 4 - 1)

    unit_loop(units3, where3, r2, 0, 1, after3)
    for_each(SHARE3, receive3, start=in_loop3)

    def drain3(q):
        local_copy(3, 1, r3, l, mine + q).wait()
        partner_copy(3, pv(1, l, mine + q), r3, l, mine + q).wait()
        partner_copy(3, pv(1, 1 - l, mine + q), r3, 1 - l, mine + q).wait()
    for_each(NC, drain3)
    for_each(NC, lambda q: local_copy(3, 1, r3, 1 - l, mine + q).wait(), start=SHARE3)
    for_each(SHARE3, lambda q: x_copy(2, own(0), pv(1, l, other + q), q).wait_recv())
    drain_sends(2, SHARE3)

    def out_copy(u, slot):
        return pltpu.make_async_copy(pv(0, l, mine + u), o_ref.at[:, cols(u)], osem.at[slot])

    def after4(u, ls, c):
        @pl.when(u > 0)
        def _():
            out_copy(u - 1, 0).wait()
        out_copy(u, 0).start()

    unit_loop(NC, lambda u: (l, mine + u), r3, 1, 0, after4)
    out_copy(NC - 1, 0).wait()


def solution(mesh):
    layout = P(('row', 'depth'), 'col')

    def step(block):
        slab, half = block.shape
        n = 2 * half
        dma = pltpu.SemaphoreType.DMA
        whole = jax.ShapeDtypeStruct((n, n), block.dtype)
        hbm = pl.BlockSpec(memory_space=pltpu.HBM)
        return pl.pallas_call(
            functools.partial(kernel, n),
            out_shape=(jax.ShapeDtypeStruct(block.shape, block.dtype),) + (whole,) * 4,
            in_specs=[hbm],
            out_specs=(hbm,) * 5,
            scratch_shapes=[
                pltpu.VMEM((2, half, n), block.dtype),
                pltpu.VMEM((2, n, n // (2 * NC)), block.dtype),
                dma((4, 4 * NC)), dma((4, 4 * NC)), dma((4, 4 * NC)),
                dma((3, NC + NC // 2)), dma((3, NC + NC // 2)),
                dma((3, NC + NC // 2)), dma((3, NC + NC // 2)),
                dma((2,)), dma((2,)), pltpu.SemaphoreType.REGULAR((2,)),
            ],
            compiler_params=pltpu.CompilerParams(
                collective_id=0, has_side_effects=True, vmem_limit_bytes=67043328),
            name='squarings',
        )(block)[0]

    return jax.shard_map(step, mesh=mesh, in_specs=(layout,), out_specs=layout, check_vma=False)
```

```python
import functools

import jax
import jax.numpy as jnp
from jax import lax
from jax.experimental import pallas as pl
from jax.experimental.pallas import tpu as pltpu
from jax.sharding import PartitionSpec as P

MESH = pl.DeviceIdType.MESH
NC = 10
NW = 5
SHARE2 = 6
SHARE3 = 5


def kernel(n, s_ref, o_ref, r0, r1, r2, r3, p0, p1, bbuf, qbuf,
           loc, ps, pr, xs, xr, ys, yr, bsem, osem, rdy):
    half, slab, width = n // 2, n // 4, n // (2 * NC)
    l = lax.axis_index('depth')
    j = lax.axis_index('col')
    i = lax.axis_index('row')
    x_dev, y_dev, p_dev = {'col': 1 - j}, {'depth': 1 - l}, {'row': 1 - i}

    def mo(v, m):
        return pl.multiple_of(v, m)

    def rows(ls):
        return pl.ds(mo(ls * slab, slab), slab)

    def cols(c, w=1):
        return pl.ds(mo(c * w * width, w * width), w * width)

    def pv(buf, ls, c, w=1):
        return buf.at[rows(ls), cols(c, w)]

    def rv(r, ls, c, w=1):
        return r.at[pl.ds(mo(i * half + ls * slab, slab), slab), cols(c, w)]

    def remote(src, dst, ssem, rsem, dev):
        return pltpu.make_async_remote_copy(
            src_ref=src, dst_ref=dst, send_sem=ssem, recv_sem=rsem, device_id=dev, device_id_type=MESH)

    def local_copy(k, buf, r, ls, c, w=1):
        return pltpu.make_async_copy(pv(buf, ls, c, w), rv(r, ls, c, w), loc.at[k, ls * 2 * NC + c])

    def partner_copy(k, src, r, ls, c, w=1):
        q = ls * 2 * NC + c
        return remote(src, rv(r, ls, c, w), ps.at[k, q], pr.at[k, q], p_dev)

    def x_copy(k, src, dst, q):
        return remote(src, dst, xs.at[k, q], xr.at[k, q], x_dev)

    def y_copy(k, src, dst, q):
        return remote(src, dst, ys.at[k, q], yr.at[k, q], y_dev)

    def publish(k, buf, r, ls, c, w=1):
        local_copy(k, buf, r, ls, c, w).start()
        partner_copy(k, pv(buf, ls, c, w), r, ls, c, w).start()

    def settle(k, buf, r, ls, c, w=1):
        local_copy(k, buf, r, ls, c, w).wait()
        partner_copy(k, pv(buf, ls, c, w), r, ls, c, w).wait_recv()

    def sent(k, buf, r, ls, c, w=1):
        partner_copy(k, pv(buf, ls, c, w), r, ls, c, w).wait_send()

    def drain_sends(k, count, ref, w):
        def body(q):
            x_copy(k, pv(ref, 0, 0, w), pv(ref, 0, 0, w), q).wait_send()
            y_copy(k, pv(ref, 0, 0, w), pv(ref, 0, 0, w), q).wait_send()
        for_each(count, body)

    def ready(k):
        for dev in (x_dev, y_dev):
            pl.semaphore_signal(rdy.at[k], inc=1, device_id=dev, device_id_type=MESH)

    def for_each(count, body, start=0):
        def step(q, carry):
            body(q)
            return carry
        lax.fori_loop(start, count, step, 0)

    mine, other = j * NC, (1 - j) * NC
    mine_w, other_w = j * NW, (1 - j) * NW

    barrier = pltpu.get_barrier_semaphore()
    for dev in (x_dev, y_dev, p_dev):
        pl.semaphore_signal(barrier, inc=1, device_id=dev, device_id_type=MESH)
    pl.semaphore_wait(barrier, 3)

    def place(p):
        return jnp.where(l == 0, p, NW - 1 - p)

    def diag_order(q):
        return 2 if q == 1 else 1 if q == 0 else 0 if q == 2 else q

    def own(c, w=2):
        return s_ref.at[:, cols(c, w)]

    def start_own(p):
        near_c, far_c = place(p), NW - 1 - place(p)
        x_copy(0, own(near_c), pv(p0, l, mine_w + near_c, 2), p).start()
        y_copy(0, own(far_c), pv(p0, l, mine_w + far_c, 2), p).start()
        partner_copy(0, own(near_c), r0, l, mine_w + near_c, 2).start()
    for_each(NW, start_own)
    own_load = pltpu.make_async_copy(s_ref, p0.at[rows(l), pl.ds(mo(j * half, half), half)], osem.at[0])
    own_load.start()

    strip = slab // 10

    def merge(ls, c, mode):
        def body(q):
            rs = pl.ds(mo(ls * slab + q * strip, strip), strip)
            if mode == 'clear':
                p1[rs, cols(c, 2)] = jnp.zeros((strip, 2 * width), jnp.bfloat16)
            elif mode == 'copy':
                p1[rs, cols(c, 2)] = p0[rs, cols(c, 2)]
            else:
                p1[rs, cols(c, 2)] = jnp.maximum(p0[rs, cols(c, 2)], p1[rs, cols(c, 2)])
        for_each(10, body)

    for_each(NW, lambda p: merge(1 - l, other_w + p, 'clear'))
    own_load.wait()
    for_each(NW, lambda p: local_copy(0, p0, r0, l, mine_w + p, 2).start())
    for_each(NW, lambda p: merge(l, mine_w + p, 'copy'))
    for_each(NW, lambda p: settle(0, p0, r0, l, mine_w + p, 2))

    def inner(ks):
        return pl.ds(mo(ks * slab, slab), slab)

    def q_copy(ks, c, slot):
        return pltpu.make_async_copy(r0.at[inner(ks), cols(c, 2)], qbuf.at[slot], bsem.at[slot])

    def partial_loop(segments, gate, gate_fn, after=None):
        total = sum(seg[0] for seg in segments)

        def where(v):
            found, start = None, 0
            for count, ls, ks, first in segments:
                here = (ls, ks, first + (v - start) * (1 - 2 * l))
                if found is None:
                    found = here
                else:
                    later = v >= start
                    found = tuple(jnp.where(later, new, old) for new, old in zip(here, found))
                start = start + count
            return found

        @pl.when(gate == 0)
        def _():
            gate_fn()
        begin = where(jnp.int32(0))
        q_copy(begin[1], begin[2], 0).start()

        def step(v, carry):
            ls, ks, c = carry
            slot = lax.rem(v, 2)
            following = where(v + 1)

            @pl.when(v + 1 == gate)
            def _():
                gate_fn()

            @pl.when(v + 1 < total)
            def _():
                q_copy(following[1], following[2], 1 - slot).start()
            q_copy(ks, c, slot).wait()
            acc = jnp.dot(p0[rows(ls), inner(ks)], qbuf[slot], preferred_element_type=jnp.float32)
            acc = acc + p1[rows(ls), cols(c, 2)].astype(jnp.float32)
            p1[rows(ls), cols(c, 2)] = jnp.minimum(acc, 1.0).astype(jnp.bfloat16)
            if after is not None:
                after(v, ls, c)
            return following
        lax.fori_loop(0, total, step, begin)

    def flag(condition):
        return condition.astype(jnp.int32)

    ja, jb, oa, ob = 2 * j + l, 2 * j + 1 - l, 2 * (1 - j) + l, 2 * (1 - j) + 1 - l
    near, far = l, 1 - l

    def relay(q):
        a = diag_order(q)
        x_c = place(a)
        y_c = NW - 1 - x_c
        x_src = p0.at[rows(1 - l), cols(2 * (mine_w + x_c))]
        y_src = p0.at[rows(l), cols(2 * (other_w + y_c) + 1)]
        x_copy(0, x_src, x_src, NW + q).start()
        y_copy(0, y_src, y_src, NW + q).start()

    def arrive(p):
        x_c, y_c = other_w + place(p), mine_w + place(p)
        x_copy(0, own(0), pv(p0, l, x_c, 2), p).wait_recv()
        publish(0, p0, r0, l, x_c, 2)
        y_copy(0, own(0), pv(p0, 1 - l, y_c, 2), p).wait_recv()
        publish(0, p0, r0, 1 - l, y_c, 2)

        @pl.when(p == 3)
        def _():
            relay(0)
            relay(1)

        @pl.when(p == 4)
        def _():
            relay(2)
            relay(3)
            relay(4)
        merge(l, x_c, 'copy')
        merge(1 - l, y_c, 'copy')

        def gate_fn():
            settle(0, p0, r0, l, x_c, 2)
            settle(0, p0, r0, 1 - l, y_c, 2)
        at_0, at_2, at_4, from_3 = flag(p == 0), flag(p == 2), flag(p == 4), flag(p > 2)
        some, first = 3 * at_2 + from_3, place(p * from_3)
        partial_loop([
            (5 * at_0, near, ja, mine_w + place(0)),
            (4 * at_4, near, ob, mine_w + place(0)),
            (1, near, ja, x_c),
            (1, near, jb, y_c),
            (5 * at_2, near, oa, mine_w + place(0)),
            (some, near, oa, other_w + first),
            (some, far, ja, mine_w + first),
            (some, far, ja, other_w + first),
            (at_4, near, ob, mine_w + place(4)),
        ], 5 * at_0 + 4 * at_4, gate_fn)
    for_each(NW, arrive)
    for_each(NW, lambda q: publish(1, p1, r1, l, mine_w + q, 2))

    def diagonal(q):
        a = jnp.where(q == 0, 1, jnp.where(q == 1, 2, jnp.where(q == 2, 0, q)))
        d = other_w + place(a)
        x_copy(0, own(0, 1), p0.at[rows(1 - l), cols(2 * d)], NW + q).wait_recv()
        y_copy(0, own(0, 1), p0.at[rows(1 - l), cols(2 * d + 1)], NW + q).wait_recv()
        publish(0, p0, r0, 1 - l, d, 2)
        merge(1 - l, d, 'max')
        at_0, at_2, at_3, at_4 = flag(q == 0), flag(q == 2), flag(q == 3), flag(q == 4)
        fill = 5 * (at_0 + at_2 + at_3 + at_4)

        def after(v, ls, c):
            @pl.when((v == fill + 1) | ((q == 4) & ((v < fill) | (v >= fill + 3))))
            def _():
                publish(1, p1, r1, ls, c, 2)
        partial_loop([
            (5 * at_0, far, jb, mine_w + place(0)),
            (5 * at_2, far, oa, mine_w + place(0)),
            (5 * at_3, far, oa, other_w + place(0)),
            (5 * at_4, far, ob, mine_w + place(0)),
            (1, near, jb, d),
            (1, near, ob, d),
            (1, far, jb, d),
            (5 * at_4, far, ob, other_w + place(0)),
        ], fill, lambda: settle(0, p0, r0, 1 - l, d, 2), after)
    for_each(NW, diagonal)

    def flush0(q):
        sent(0, p0, r0, 0, q, 2)
        sent(0, p0, r0, 1, q, 2)
    for_each(2 * NW, flush0)
    drain_sends(0, NW, p0, 2)

    def flush_relays(q):
        x_copy(0, pv(p0, 0, 0), pv(p0, 0, 0), NW + q).wait_send()
        y_copy(0, pv(p0, 0, 0), pv(p0, 0, 0), NW + q).wait_send()
    for_each(NW, flush_relays)
    ready(0)

    def unit_loop(count, where, r, src, dst, before, after):
        def b_copy(c, slot):
            return pltpu.make_async_copy(r.at[:, cols(c)], bbuf.at[slot], bsem.at[slot])

        before(jnp.int32(0))
        b_copy(where(0)[1], 0).start()

        def body(u):
            slot = lax.rem(u, 2)
            ls, c = where(u)

            @pl.when(u + 1 < count)
            def _():
                before(u + 1)
                b_copy(where(u + 1)[1], 1 - slot).start()
            b_copy(c, slot).wait()
            acc = jnp.dot(src[rows(ls), :], bbuf[slot], preferred_element_type=jnp.float32)
            old = src[rows(ls), cols(c)].astype(jnp.float32)
            dst[rows(ls), cols(c)] = jnp.minimum(acc + old, 1.0).astype(jnp.bfloat16)
            after(u, ls, c)
        for_each(count, body)

    def where2(u):
        first = u < NC
        second = u < 2 * NC
        third = u < 3 * NC - SHARE2
        ls = jnp.where(first | (~second & third), l, 1 - l)
        c = jnp.where(first, mine + u, jnp.where(second, other + u - NC, jnp.where(
            third, other + SHARE2 + u - 2 * NC, mine + 2 * SHARE2 + u - 3 * NC)))
        return ls, c

    def before2(u):
        @pl.when((u < 2 * NC) & (lax.rem(u, 2) == 0))
        def _():
            c = jnp.where(u < NC, mine_w + u // 2, other_w + u // 2 - NW)
            for ls in (0, 1):
                settle(1, p1, r1, ls, c, 2)

    def receive2(q):
        x_copy(1, pv(p0, l, mine), pv(p0, l, other + q), q).wait_recv()
        publish(2, p0, r2, l, other + q)
        y_copy(1, pv(p0, l, mine), pv(p0, 1 - l, mine + q), q).wait_recv()
        publish(2, p0, r2, 1 - l, mine + q)

    units2 = 4 * NC - 2 * SHARE2
    in_loop2 = min(SHARE2, units2 // 4 - 1)

    def after2(u, ls, c):
        publish(2, p0, r2, ls, c)

        @pl.when(u == 0)
        def _():
            pl.semaphore_wait(rdy.at[0], 2)

        @pl.when(u < SHARE2)
        def _():
            x_copy(1, pv(p0, l, mine + u), pv(p0, l, mine + u), u).start()
            y_copy(1, pv(p0, l, mine + u), pv(p0, l, mine + u), u).start()

        @pl.when((lax.rem(u, 4) == 3) & (u >= 4) & (u // 4 - 1 < in_loop2))
        def _():
            receive2(u // 4 - 1)

    unit_loop(units2, where2, r1, p1, p0, before2, after2)
    for_each(SHARE2, receive2, start=in_loop2)

    def flush1(q):
        sent(1, p1, r1, 0, q, 2)
        sent(1, p1, r1, 1, q, 2)
    for_each(2 * NW, flush1)
    ready(1)

    def where3(u):
        first = u < NC
        second = u < 2 * NC - SHARE3
        ls = jnp.where(second, l, 1 - l)
        c = jnp.where(first, mine + u, jnp.where(second, other + SHARE3 + u - NC, mine + 2 * SHARE3 + u - 2 * NC))
        return ls, c

    def before3(u):
        @pl.when(u < 2 * NC - SHARE3)
        def _():
            for ls in (0, 1):
                settle(2, p0, r2, ls, where3(u)[1])

    def receive3(q):
        y_copy(2, pv(p1, l, mine), rv(r3, 1 - l, mine + q), q).wait_recv()
        partner_copy(3, rv(r3, 1 - l, mine + q), r3, 1 - l, mine + q).start()

    units3 = 3 * NC - 2 * SHARE3
    in_loop3 = min(SHARE3, units3 // 4 - 1)

    def after3(u, ls, c):
        @pl.when((u < NC) | (u >= 2 * NC - SHARE3))
        def _():
            publish(3, p1, r3, ls, c)

        @pl.when(u == 0)
        def _():
            pl.semaphore_wait(rdy.at[1], 2)

        @pl.when(u < SHARE3)
        def _():
            x_copy(2, pv(p1, l, mine + u), pv(p1, l, mine + u), u).start()
            y_copy(2, pv(p1, l, mine + u), rv(r3, l, mine + u), u).start()

        @pl.when((lax.rem(u, 4) == 3) & (u >= 4) & (u // 4 - 1 < in_loop3))
        def _():
            receive3(u // 4 - 1)

    unit_loop(units3, where3, r2, p0, p1, before3, after3)
    for_each(SHARE3, receive3, start=in_loop3)
    for_each(SHARE3, lambda q: x_copy(2, pv(p1, l, mine), pv(p1, l, other + q), q).wait_recv())

    def flush2(q):
        sent(2, p0, r2, 0, q)
        sent(2, p0, r2, 1, q)
    for_each(2 * NC, flush2)
    drain_sends(1, SHARE2, p0, 1)

    def unused2(q):
        settle(2, p0, r2, 0, other + q)
        settle(2, p0, r2, 1, other + q)
    for_each(SHARE3, unused2)

    def before4(u):
        settle(3, p1, r3, l, mine + u)
        partner_copy(3, pv(p1, 1 - l, mine + u), r3, 1 - l, mine + u).wait_recv()

        @pl.when(u >= SHARE3)
        def _():
            local_copy(3, p1, r3, 1 - l, mine + u).wait()

    def out_copy(u, slot):
        return pltpu.make_async_copy(pv(p0, l, mine + u), o_ref.at[:, cols(u)], osem.at[slot])

    def after4(u, ls, c):
        @pl.when(u > 0)
        def _():
            out_copy(u - 1, 0).wait()
        out_copy(u, 0).start()

    unit_loop(NC, lambda u: (l, mine + u), r3, p1, p0, before4, after4)

    def flush3(q):
        sent(3, p1, r3, 0, mine + q)
        sent(3, p1, r3, 1, mine + q)
    for_each(NC, flush3)
    drain_sends(2, SHARE3, p1, 1)
    out_copy(NC - 1, 0).wait()


def solution(mesh):
    layout = P(('row', 'depth'), 'col')

    def step(block):
        slab, half = block.shape
        n = 2 * half
        dma = pltpu.SemaphoreType.DMA
        whole = jax.ShapeDtypeStruct((n, n), block.dtype)
        hbm = pl.BlockSpec(memory_space=pltpu.HBM)
        return pl.pallas_call(
            functools.partial(kernel, n),
            out_shape=(jax.ShapeDtypeStruct(block.shape, block.dtype),) + (whole,) * 4,
            in_specs=[hbm],
            out_specs=(hbm,) * 5,
            scratch_shapes=[
                pltpu.VMEM((half, n), block.dtype),
                pltpu.VMEM((half, n), block.dtype),
                pltpu.VMEM((2, n, n // (2 * NC)), block.dtype),
                pltpu.VMEM((2, slab, n // (2 * NW)), block.dtype),
                dma((4, 4 * NC)), dma((4, 4 * NC)), dma((4, 4 * NC)),
                dma((3, NC)), dma((3, NC)), dma((3, NC)), dma((3, NC)),
                dma((2,)), dma((2,)), pltpu.SemaphoreType.REGULAR((2,)),
            ],
            compiler_params=pltpu.CompilerParams(
                collective_id=0, has_side_effects=True, vmem_limit_bytes=67043328),
            name='squarings',
        )(block)[0]

    return jax.shard_map(step, mesh=mesh, in_specs=(layout,), out_specs=layout, check_vma=False)
```

```python
import functools

import jax
import jax.numpy as jnp
from jax import lax
from jax.experimental import pallas as pl
from jax.experimental.pallas import tpu as pltpu
from jax.sharding import PartitionSpec as P

MESH = pl.DeviceIdType.MESH
NC = 10
NW = 5
X2, Y2 = 3, 4
X3, Y3 = 2, 2
OWN3 = (0, 1, 2, 4, 3)
OWN4 = (0, 2, 3, 1, 4)


def kernel(n, s_ref, o_ref, r0, r1, r2, r3, p0, p1, bbuf,
           loc, ps, pr, xs, xr, ys, yr, bsem, osem, rdy):
    half, slab, width = n // 2, n // 4, n // (2 * NC)
    l = lax.axis_index('depth')
    j = lax.axis_index('col')
    i = lax.axis_index('row')
    x_dev, y_dev, p_dev = {'col': 1 - j}, {'depth': 1 - l}, {'row': 1 - i}

    def mo(v, m):
        return pl.multiple_of(v, m)

    def rows(ls):
        return pl.ds(mo(ls * slab, slab), slab)

    def cols(c, w=1):
        return pl.ds(mo(c * w * width, w * width), w * width)

    def pv(buf, ls, c, w=1):
        return buf.at[rows(ls), cols(c, w)]

    def rv(r, ls, c, w=1):
        return r.at[pl.ds(mo(i * half + ls * slab, slab), slab), cols(c, w)]

    def remote(src, dst, ssem, rsem, dev):
        return pltpu.make_async_remote_copy(
            src_ref=src, dst_ref=dst, send_sem=ssem, recv_sem=rsem, device_id=dev, device_id_type=MESH)

    def local_copy(k, buf, r, ls, c):
        return pltpu.make_async_copy(pv(buf, ls, c, 2), rv(r, ls, c, 2), loc.at[k, ls * 2 * NW + c])

    def partner_copy(k, src, r, ls, c):
        return remote(src, rv(r, ls, c, 2), ps.at[k], pr.at[k, ls * 2 * NW + c], p_dev)

    def x_copy(k, src, dst, q):
        return remote(src, dst, xs.at[k], xr.at[(0, NC, NC + NW)[k] + q], x_dev)

    def y_copy(k, src, dst, q):
        return remote(src, dst, ys.at[k], yr.at[(0, NC, NC + NW)[k] + q], y_dev)

    def publish(k, buf, r, ls, c):
        local_copy(k, buf, r, ls, c).start()
        partner_copy(k, pv(buf, ls, c, 2), r, ls, c).start()

    def settle(k, buf, r, ls, c):
        local_copy(k, buf, r, ls, c).wait()
        partner_copy(k, pv(buf, ls, c, 2), r, ls, c).wait_recv()

    def partner_sent(k, buf, count):
        part = buf.at[:, pl.ds(0, count * width)]
        remote(part, part, ps.at[k], pr.at[k, 0], p_dev).wait_send()

    def sent(copy, k, buf, count):
        part = buf.at[rows(0), pl.ds(0, count * width)]
        copy(k, part, part, 0).wait_send()

    def ready(k):
        for dev in (x_dev, y_dev):
            pl.semaphore_signal(rdy.at[k], inc=1, device_id=dev, device_id_type=MESH)

    def for_each(count, body, start=0):
        def step(q, carry):
            body(q)
            return carry
        lax.fori_loop(start, count, step, 0)

    mine, other = j * NC, (1 - j) * NC
    mine_w, other_w = j * NW, (1 - j) * NW

    barrier = pltpu.get_barrier_semaphore()
    for dev in (x_dev, y_dev, p_dev):
        pl.semaphore_signal(barrier, inc=1, device_id=dev, device_id_type=MESH)
    pl.semaphore_wait(barrier, 3)

    def place(p):
        return jnp.where(l == 0, p, NW - 1 - p)

    def diag_order(q):
        return 2 if q == 1 else 1 if q == 0 else 0 if q == 2 else q

    def own(c, w=2):
        return s_ref.at[:, cols(c, w)]

    def start_own(p):
        near_c, far_c = place(p), NW - 1 - place(p)
        x_copy(0, own(near_c), pv(p0, l, mine_w + near_c, 2), p).start()
        y_copy(0, own(far_c), pv(p0, l, mine_w + far_c, 2), p).start()
        partner_copy(0, own(near_c), r0, l, mine_w + near_c).start()
    for_each(NW, start_own)
    own_load = pltpu.make_async_copy(s_ref, p0.at[rows(l), pl.ds(mo(j * half, half), half)], osem.at[0])
    own_load.start()

    strip = slab // 10

    def merge(ls, c, mode):
        def body(q):
            rs = pl.ds(mo(ls * slab + q * strip, strip), strip)
            if mode == 'clear':
                p1[rs, cols(c, 2)] = jnp.zeros((strip, 2 * width), jnp.bfloat16)
            elif mode == 'copy':
                p1[rs, cols(c, 2)] = p0[rs, cols(c, 2)]
            else:
                p1[rs, cols(c, 2)] = jnp.maximum(p0[rs, cols(c, 2)], p1[rs, cols(c, 2)])
        for_each(10, body)

    for_each(NW, lambda p: merge(1 - l, other_w + p, 'clear'))
    own_load.wait()
    for_each(NW, lambda p: local_copy(0, p0, r0, l, mine_w + p).start())
    for_each(NW, lambda p: merge(l, mine_w + p, 'copy'))
    for_each(NW, lambda p: settle(0, p0, r0, l, mine_w + p))

    def inner(ks):
        return pl.ds(mo(ks * slab, slab), slab)

    def q_copy(ks, c, slot):
        return pltpu.make_async_copy(r0.at[inner(ks), cols(c, 2)], bbuf.at[slot, pl.ds(0, slab), :], bsem.at[slot])

    def partial_loop(segments, total, first_gated, arrive_fn, before, after=None):
        def where(v):
            found, start = None, 0
            for count, ls, ks, first, stride in segments:
                here = (ls, ks, first + (v - start) * stride)
                if found is None:
                    found = here
                else:
                    later = v >= start
                    found = tuple(jnp.where(later, new, old) for new, old in zip(here, found))
                start = start + count
            return found

        begin = where(jnp.int32(0))

        @pl.when(jnp.logical_not(first_gated))
        def _():
            q_copy(begin[1], begin[2], 0).start()
        arrive_fn()
        before(jnp.int32(0))

        @pl.when(first_gated)
        def _():
            q_copy(begin[1], begin[2], 0).start()

        def step(v, carry):
            ls, ks, c = carry
            slot = lax.rem(v, 2)
            following = where(v + 1)
            before(v + 1)

            @pl.when(v + 1 < total)
            def _():
                q_copy(following[1], following[2], 1 - slot).start()
            q_copy(ks, c, slot).wait()
            acc = jnp.dot(p0[rows(ls), inner(ks)], bbuf[slot, pl.ds(0, slab), :], preferred_element_type=jnp.float32)
            acc = acc + p1[rows(ls), cols(c, 2)].astype(jnp.float32)
            p1[rows(ls), cols(c, 2)] = jnp.minimum(acc, 1.0).astype(jnp.bfloat16)
            if after is not None:
                after(v, ls, c)
            return following
        lax.fori_loop(0, total, step, begin)

    def flag(condition):
        return condition.astype(jnp.int32)

    ja, jb, oa, ob = 2 * j + l, 2 * j + 1 - l, 2 * (1 - j) + l, 2 * (1 - j) + 1 - l
    near, far = l, 1 - l

    def relay(q):
        a = diag_order(q)
        x_c = place(a)
        y_c = NW - 1 - x_c
        x_src = p0.at[rows(1 - l), cols(2 * (mine_w + x_c))]
        y_src = p0.at[rows(l), cols(2 * (other_w + y_c) + 1)]
        x_copy(0, x_src, x_src, NW + q).start()
        y_copy(0, y_src, y_src, NW + q).start()

    def arrive(p):
        x_c, y_c = other_w + place(p), mine_w + place(p)

        def arrive_fn():
            x_copy(0, own(0), pv(p0, l, x_c, 2), p).wait_recv()
            publish(0, p0, r0, l, x_c)
            y_copy(0, own(0), pv(p0, 1 - l, y_c, 2), p).wait_recv()
            publish(0, p0, r0, 1 - l, y_c)

            @pl.when(p == 3)
            def _():
                relay(0)
                relay(1)

            @pl.when(p == 4)
            def _():
                relay(2)
                relay(3)
                relay(4)
            merge(l, x_c, 'copy')
            merge(1 - l, y_c, 'copy')

        at_0, at_2, at_4, from_3 = flag(p == 0), flag(p == 2), flag(p == 4), flag(p > 2)
        some, first, way = 3 * at_2 + from_3, place(p * from_3), 1 - 2 * l
        gate = 5 * at_0 + 4 * at_4

        def before(v):
            @pl.when(v == gate)
            def _():
                settle(0, p0, r0, l, x_c)
                settle(0, p0, r0, 1 - l, y_c)
        partial_loop([
            (5 * at_0, near, ja, mine_w, 1),
            (4 * at_4, near, ob, mine_w + place(0), way),
            (1, near, ja, x_c, 1),
            (1, near, jb, y_c, 1),
            (5 * at_2, near, oa, mine_w, 1),
            (some, near, oa, other_w + first, way),
            (some, far, ja, mine_w + first, way),
            (some, far, ja, other_w + first, way),
            (at_4, near, ob, mine_w + place(4), 1),
        ], gate + 2 + 5 * at_2 + 3 * some + at_4, gate == 0, arrive_fn, before)
    for_each(NW, arrive)
    for_each(NW, lambda q: publish(1, p1, r1, l, mine_w + q))

    def diag_column(q):
        a = jnp.where(q == 0, 1, jnp.where(q == 1, 2, jnp.where(q == 2, 0, q)))
        return other_w + place(a)

    def diag_arrive(q):
        d = diag_column(q)
        x_copy(0, own(0, 1), p0.at[rows(1 - l), cols(2 * d)], NW + q).wait_recv()
        y_copy(0, own(0, 1), p0.at[rows(1 - l), cols(2 * d + 1)], NW + q).wait_recv()
        publish(0, p0, r0, 1 - l, d)
        merge(1 - l, d, 'max')

    def d_copy(base, v, slot):
        return pltpu.make_async_copy(
            r0.at[pl.ds(mo((1 - j) * half, half), half), cols(base + v, 2)],
            bbuf.at[slot, pl.ds(0, half), :], bsem.at[slot])

    def b_copy(r, c, slot):
        return pltpu.make_async_copy(r.at[:, cols(c, 2)], bbuf.at[slot], bsem.at[slot])

    def on(v, values, body):
        hit = v == values[0]
        for value in values[1:]:
            hit = hit | (v == value)

        @pl.when(hit)
        def _():
            body()

    def before_diag(v):
        for q, arrival, reading in ((0, None, 5), (1, 4, 8), (2, 11, 16), (3, 17, 19), (4, 23, 27)):
            if arrival is not None:
                on(v, (arrival,), lambda: diag_arrive(q))
            on(v, (reading,), lambda: settle(0, p0, r0, 1 - l, diag_column(q)))

        @pl.when(v == 30)
        def _():
            for ls in (0, 1):
                settle(1, p1, r1, ls, mine_w)
            b_copy(r1, mine_w, 0).start()

    def after_diag(v, ls, c):
        on(v, (6, 9, 17, 20, 28, 22, 23, 24, 25, 26), lambda: publish(1, p1, r1, ls, c))

    def pieces(q):
        d = diag_column(q)
        return [(1, near, jb, d, 1), (1, near, ob, d, 1), (1, far, jb, d, 1)]
    partial_loop(
        [(NW, far, jb, mine_w, 1)] + pieces(0) + pieces(1) + [(NW, far, oa, mine_w, 1)]
        + pieces(2) + pieces(3) + [(NW, far, ob, mine_w, 1)] + pieces(4),
        30, jnp.bool_(False), lambda: diag_arrive(0), before_diag, after_diag)

    partner_sent(0, p0, 4 * NW)
    sent(x_copy, 0, p0, 3 * NW)
    sent(y_copy, 0, p0, 3 * NW)
    ready(0)

    def deep_loop(base, after, tail):
        span = pl.ds(mo((1 - j) * half, half), half)

        def step(v):
            slot = lax.rem(v + 1, 2)

            @pl.when(v + 1 < NW)
            def _():
                d_copy(base, v + 1, 1 - slot).start()

            @pl.when(v + 1 == NW)
            def _():
                tail()
            d_copy(base, v, slot).wait()
            c = base + v
            acc = jnp.dot(p0[rows(1 - l), span], bbuf[slot, pl.ds(0, half), :], preferred_element_type=jnp.float32)
            acc = acc + p1[rows(1 - l), cols(c, 2)].astype(jnp.float32)
            p1[rows(1 - l), cols(c, 2)] = jnp.minimum(acc, 1.0).astype(jnp.bfloat16)
            after(c)
        for_each(NW, step)

    def unit_loop(start, stop, shift, where, r, src, dst, before, after, tail):
        def body(u):
            slot = lax.rem(u + shift, 2)
            ls, c = where(u)

            @pl.when(u + 1 < stop)
            def _():
                before(u + 1)
                b_copy(r, where(u + 1)[1], 1 - slot).start()

            @pl.when(u + 1 == stop)
            def _():
                tail()
            b_copy(r, c, slot).wait()
            acc = jnp.dot(src[rows(ls), :], bbuf[slot], preferred_element_type=jnp.float32)
            old = src[rows(ls), cols(c, 2)].astype(jnp.float32)
            dst[rows(ls), cols(c, 2)] = jnp.minimum(acc + old, 1.0).astype(jnp.bfloat16)
            after(u, ls, c)
        for_each(stop, body, start=start)

    def pick(u, table):
        found = table[-1]
        for index, value in enumerate(table[:-1]):
            found = jnp.where(u == index, value, found)
        return found

    def where2(u):
        own_u, diag_u, near_u = u < NW, u < 2 * NW, u < 3 * NW - X2
        ls = jnp.where(own_u | (~diag_u & near_u), l, 1 - l)
        c = jnp.where(own_u, mine_w + u, jnp.where(diag_u, other_w + u - NW, jnp.where(
            near_u, other_w + X2 + u - 2 * NW, mine_w + Y2 + u - 3 * NW + X2)))
        return ls, c

    def before2(u):
        @pl.when(u < 2 * NW)
        def _():
            for ls in (0, 1):
                settle(1, p1, r1, ls, where2(u)[1])

    def receive2_x(q):
        x_copy(1, pv(p0, l, mine_w, 2), pv(p0, l, other_w + q, 2), q).wait_recv()
        publish(2, p0, r2, l, other_w + q)

    def receive2_y(q):
        y_copy(1, pv(p0, l, mine_w, 2), pv(p0, 1 - l, mine_w + q, 2), q).wait_recv()
        publish(2, p0, r2, 1 - l, mine_w + q)

    def after2(u, ls, c):
        publish(2, p0, r2, ls, c)

        @pl.when(u == 0)
        def _():
            pl.semaphore_wait(rdy.at[0], 2)

        for copy, share in ((x_copy, X2), (y_copy, Y2)):
            @pl.when(u < share)
            def _():
                copy(1, pv(p0, l, mine_w + u, 2), pv(p0, l, mine_w + u, 2), u).start()

        for q, when in enumerate((5, 7, 11)):
            @pl.when(u == when)
            def _():
                receive2_x(q)
                receive2_y(q)

    def where3(u):
        own_u, near_u = u < NW, u < 2 * NW - X3
        ls = jnp.where(near_u, l, 1 - l)
        c = jnp.where(own_u, mine_w + pick(u, OWN3), jnp.where(
            near_u, other_w + X3 + u - NW, mine_w + Y3 + u - 2 * NW + X3))
        return ls, c

    def before3(u):
        @pl.when(u < 2 * NW - X3)
        def _():
            for ls in (0, 1):
                settle(2, p0, r2, ls, where3(u)[1])

    def receive3(q):
        landed = rv(r3, 1 - l, mine_w + q, 2)
        y_copy(2, pv(p1, l, mine_w, 2), landed, q).wait_recv()
        partner_copy(3, landed, r3, 1 - l, mine_w + q).start()

    def after3(u, ls, c):
        @pl.when((u < NW) | (u >= 2 * NW - X3))
        def _():
            publish(3, p1, r3, ls, c)

        @pl.when(u == 0)
        def _():
            pl.semaphore_wait(rdy.at[1], 2)

        @pl.when(u < X3)
        def _():
            x_copy(2, pv(p1, l, mine_w + u, 2), pv(p1, l, mine_w + u, 2), u).start()

        @pl.when(u < Y3)
        def _():
            y_copy(2, pv(p1, l, mine_w + u, 2), rv(r3, l, mine_w + u, 2), u).start()

        @pl.when(u == 1)
        def _():
            receive2_y(3)

        @pl.when(u == 6)
        def _():
            receive3(0)

    def where4(u):
        return l, mine_w + pick(u, OWN4)

    def before4(u):
        c = where4(u)[1]
        settle(3, p1, r3, l, c)
        partner_copy(3, pv(p1, 1 - l, c, 2), r3, 1 - l, c).wait_recv()

        @pl.when(c >= mine_w + Y3)
        def _():
            local_copy(3, p1, r3, 1 - l, c).wait()

    def out_copy(u):
        c = where4(u)[1]
        return pltpu.make_async_copy(pv(p0, l, c, 2), o_ref.at[:, cols(c - mine_w, 2)], osem.at[0])

    def after4(u, ls, c):
        @pl.when(u > 0)
        def _():
            out_copy(u - 1).wait()
        out_copy(u).start()

    def read(r, where, before, u, slot):
        def start():
            before(jnp.int32(u))
            b_copy(r, where(jnp.int32(u))[1], slot).start()
        return start

    def no_tail():
        pass

    end2, end3 = 4 * NW - X2 - Y2, 3 * NW - X3 - Y3
    unit_loop(0, NW, 0, where2, r1, p1, p0, before2, after2, lambda: d_copy(other_w, 0, NW % 2).start())
    deep_loop(other_w, lambda c: publish(1, p1, r1, 1 - l, c), read(r1, where2, before2, NW, 0))
    unit_loop(NW, end2, 1, where2, r1, p1, p0, before2, after2, read(r2, where3, before3, 0, (end2 + 1) % 2))
    partner_sent(1, p1, 4 * NW)
    ready(1)
    shift3 = (end2 + 1) % 2
    unit_loop(0, end3, shift3, where3, r2, p0, p1, before3, after3, read(r3, where4, before4, 0, (end3 + shift3) % 2))
    receive3(1)
    for_each(X3, lambda q: x_copy(2, pv(p1, l, mine_w, 2), pv(p1, l, other_w + q, 2), q).wait_recv())
    partner_sent(2, p0, 4 * NW)
    sent(x_copy, 1, p0, 2 * X2)
    sent(y_copy, 1, p0, 2 * Y2)

    def unused2(q):
        settle(2, p0, r2, 0, other_w + q)
        settle(2, p0, r2, 1, other_w + q)
    for_each(X3, unused2)
    unit_loop(0, NW, (end3 + shift3) % 2, where4, r3, p1, p0, before4, after4, no_tail)
    partner_sent(3, p1, 2 * NW)
    sent(x_copy, 2, p1, 2 * X3)
    sent(y_copy, 2, p1, 2 * Y3)
    out_copy(NW - 1).wait()


def solution(mesh):
    layout = P(('row', 'depth'), 'col')

    def step(block):
        slab, half = block.shape
        n = 2 * half
        dma = pltpu.SemaphoreType.DMA
        whole = jax.ShapeDtypeStruct((n, n), block.dtype)
        hbm = pl.BlockSpec(memory_space=pltpu.HBM)
        return pl.pallas_call(
            functools.partial(kernel, n),
            out_shape=(jax.ShapeDtypeStruct(block.shape, block.dtype),) + (whole,) * 4,
            in_specs=[hbm],
            out_specs=(hbm,) * 5,
            scratch_shapes=[
                pltpu.VMEM((half, n), block.dtype),
                pltpu.VMEM((half, n), block.dtype),
                pltpu.VMEM((2, n, n // (2 * NW)), block.dtype),
                dma((4, 4 * NW)), dma((4,)), dma((4, 4 * NW)),
                dma((3,)), dma((NC + 2 * NW,)), dma((3,)), dma((NC + 2 * NW,)),
                dma((2,)), dma((1,)), pltpu.SemaphoreType.REGULAR((2,)),
            ],
            compiler_params=pltpu.CompilerParams(
                collective_id=0, has_side_effects=True, vmem_limit_bytes=67043328),
            name='squarings',
        )(block)[0]

    return jax.shard_map(step, mesh=mesh, in_specs=(layout,), out_specs=layout, check_vma=False)
```

```python
import functools

import jax
import jax.numpy as jnp
from jax import lax
from jax.experimental import pallas as pl
from jax.experimental.pallas import tpu as pltpu
from jax.sharding import PartitionSpec as P

MESH = pl.DeviceIdType.MESH
NC = 10
NW = 5
X2, Y2 = 3, 4
X3, Y3 = 2, 2
OWN3 = (0, 1, 2, 4, 3)
OWN4 = (0, 3, 4, 1, 2)


def kernel(n, s_ref, o_ref, r0, r1, r2, r3, p0, p1, bbuf,
           loc, ps, pr, xs, xr, ys, yr, bsem, psem, osem, rdy):
    half, slab, width = n // 2, n // 4, n // (2 * NC)
    l = lax.axis_index('depth')
    j = lax.axis_index('col')
    i = lax.axis_index('row')
    x_dev, y_dev, p_dev = {'col': 1 - j}, {'depth': 1 - l}, {'row': 1 - i}

    def mo(v, m):
        return pl.multiple_of(v, m)

    def rows(ls):
        return pl.ds(mo(ls * slab, slab), slab)

    def cols(c, w=1):
        return pl.ds(mo(c * w * width, w * width), w * width)

    def pv(buf, ls, c, w=1):
        return buf.at[rows(ls), cols(c, w)]

    def rv(r, ls, c, w=1):
        return r.at[pl.ds(mo(i * half + ls * slab, slab), slab), cols(c, w)]

    def remote(src, dst, ssem, rsem, dev):
        return pltpu.make_async_remote_copy(
            src_ref=src, dst_ref=dst, send_sem=ssem, recv_sem=rsem, device_id=dev, device_id_type=MESH)

    def local_copy(k, buf, r, ls, c):
        return pltpu.make_async_copy(pv(buf, ls, c, 2), rv(r, ls, c, 2), loc.at[k, ls * 2 * NW + c])

    def partner_copy(k, src, r, ls, c):
        return remote(src, rv(r, ls, c, 2), ps.at[k], pr.at[k, ls * 2 * NW + c], p_dev)

    def x_copy(k, src, dst, q):
        return remote(src, dst, xs.at[k], xr.at[(0, NC, NC + NW)[k] + q], x_dev)

    def y_copy(k, src, dst, q):
        return remote(src, dst, ys.at[k], yr.at[(0, NC, NC + NW)[k] + q], y_dev)

    def publish(k, buf, r, ls, c):
        local_copy(k, buf, r, ls, c).start()
        partner_copy(k, pv(buf, ls, c, 2), r, ls, c).start()

    def settle(k, buf, r, ls, c):
        local_copy(k, buf, r, ls, c).wait()
        partner_copy(k, pv(buf, ls, c, 2), r, ls, c).wait_recv()

    def partner_sent(k, buf, count):
        part = buf.at[:, pl.ds(0, count * width)]
        remote(part, part, ps.at[k], pr.at[k, 0], p_dev).wait_send()

    def sent(copy, k, buf, count):
        part = buf.at[rows(0), pl.ds(0, count * width)]
        copy(k, part, part, 0).wait_send()

    def ready(k):
        for dev in (x_dev, y_dev):
            pl.semaphore_signal(rdy.at[k], inc=1, device_id=dev, device_id_type=MESH)

    def for_each(count, body, start=0):
        def step(q, carry):
            body(q)
            return carry
        lax.fori_loop(start, count, step, 0)

    mine, other = j * NC, (1 - j) * NC
    mine_w, other_w = j * NW, (1 - j) * NW

    barrier = pltpu.get_barrier_semaphore()
    for dev in (x_dev, y_dev, p_dev):
        pl.semaphore_signal(barrier, inc=1, device_id=dev, device_id_type=MESH)
    pl.semaphore_wait(barrier, 3)

    def place(p):
        return jnp.where(l == 0, p, NW - 1 - p)

    def diag_order(q):
        return 2 if q == 1 else 1 if q == 0 else 0 if q == 2 else q

    def own(c, w=2):
        return s_ref.at[:, cols(c, w)]

    def start_own(p):
        near_c, far_c = place(p), NW - 1 - place(p)
        x_copy(0, own(near_c), pv(p0, l, mine_w + near_c, 2), p).start()
        y_copy(0, own(far_c), pv(p0, l, mine_w + far_c, 2), p).start()
        partner_copy(0, own(near_c), r0, l, mine_w + near_c).start()
    for_each(NW, start_own)
    own_load = pltpu.make_async_copy(s_ref, p0.at[rows(l), pl.ds(mo(j * half, half), half)], osem.at[0])
    own_load.start()

    strip = slab // 10

    def merge(ls, c, mode):
        def body(q):
            rs = pl.ds(mo(ls * slab + q * strip, strip), strip)
            if mode == 'clear':
                p1[rs, cols(c, 2)] = jnp.zeros((strip, 2 * width), jnp.bfloat16)
            elif mode == 'copy':
                p1[rs, cols(c, 2)] = p0[rs, cols(c, 2)]
            else:
                p1[rs, cols(c, 2)] = jnp.maximum(p0[rs, cols(c, 2)], p1[rs, cols(c, 2)])
        for_each(10, body)

    for_each(NW, lambda p: merge(1 - l, other_w + p, 'clear'))
    own_load.wait()
    for_each(NW, lambda p: local_copy(0, p0, r0, l, mine_w + p).start())
    for_each(NW, lambda p: merge(l, mine_w + p, 'copy'))
    for_each(NW, lambda p: settle(0, p0, r0, l, mine_w + p))

    def inner(ks):
        return pl.ds(mo(ks * slab, slab), slab)

    def q_copy(ks, c, slot):
        return pltpu.make_async_copy(r0.at[inner(ks), cols(c, 2)], bbuf.at[slot, pl.ds(0, slab), :], bsem.at[slot])

    def unit_table(segments):
        def where(v):
            found, start = None, 0
            for count, ls, ks, first, stride in segments:
                here = (ls, ks, first + (v - start) * stride)
                if found is None:
                    found = here
                else:
                    later = v >= start
                    found = tuple(jnp.where(later, new, old) for new, old in zip(here, found))
                start = start + count
            return found
        return where

    def partial_loop(segments, total, first_gated, arrive_fn, before, after=None):
        where = unit_table(segments)
        begin = where(jnp.int32(0))

        @pl.when(jnp.logical_not(first_gated))
        def _():
            q_copy(begin[1], begin[2], 0).start()
        arrive_fn()
        before(jnp.int32(0))

        @pl.when(first_gated)
        def _():
            q_copy(begin[1], begin[2], 0).start()

        def step(v, carry):
            ls, ks, c = carry
            slot = lax.rem(v, 2)
            following = where(v + 1)
            before(v + 1)

            @pl.when(v + 1 < total)
            def _():
                q_copy(following[1], following[2], 1 - slot).start()
            q_copy(ks, c, slot).wait()
            acc = jnp.dot(p0[rows(ls), inner(ks)], bbuf[slot, pl.ds(0, slab), :], preferred_element_type=jnp.float32)
            acc = acc + p1[rows(ls), cols(c, 2)].astype(jnp.float32)
            p1[rows(ls), cols(c, 2)] = jnp.minimum(acc, 1.0).astype(jnp.bfloat16)
            if after is not None:
                after(v, ls, c)
            return following
        lax.fori_loop(0, total, step, begin)

    def flag(condition):
        return condition.astype(jnp.int32)

    ja, jb, oa, ob = 2 * j + l, 2 * j + 1 - l, 2 * (1 - j) + l, 2 * (1 - j) + 1 - l
    near, far = l, 1 - l

    def relay(q):
        a = diag_order(q)
        x_c = place(a)
        y_c = NW - 1 - x_c
        x_src = p0.at[rows(1 - l), cols(2 * (mine_w + x_c))]
        y_src = p0.at[rows(l), cols(2 * (other_w + y_c) + 1)]
        x_copy(0, x_src, x_src, NW + q).start()
        y_copy(0, y_src, y_src, NW + q).start()

    def diag_column(q):
        a = jnp.where(q == 0, 1, jnp.where(q == 1, 2, jnp.where(q == 2, 0, q)))
        return other_w + place(a)

    def diag_arrive(q):
        d = diag_column(q)
        x_copy(0, own(0, 1), p0.at[rows(1 - l), cols(2 * d)], NW + q).wait_recv()
        y_copy(0, own(0, 1), p0.at[rows(1 - l), cols(2 * d + 1)], NW + q).wait_recv()
        publish(0, p0, r0, 1 - l, d)
        merge(1 - l, d, 'max')

    def arrive(p):
        x_c, y_c = other_w + place(p), mine_w + place(p)

        def arrive_fn():
            x_copy(0, own(0), pv(p0, l, x_c, 2), p).wait_recv()
            publish(0, p0, r0, l, x_c)
            y_copy(0, own(0), pv(p0, 1 - l, y_c, 2), p).wait_recv()
            publish(0, p0, r0, 1 - l, y_c)

            @pl.when(p == 3)
            def _():
                relay(0)
                relay(1)

            @pl.when(p == 4)
            def _():
                relay(2)
                relay(3)
                relay(4)
            merge(l, x_c, 'copy')
            merge(1 - l, y_c, 'copy')

        at_0, at_2, at_4, from_3 = flag(p == 0), flag(p == 2), flag(p == 4), flag(p > 2)
        some, first, way = 3 * at_2 + from_3, place(p * from_3), 1 - 2 * l
        gate = 5 * at_0 + 4 * at_4

        def before(v):
            @pl.when(v == gate)
            def _():
                settle(0, p0, r0, l, x_c)
                settle(0, p0, r0, 1 - l, y_c)

            @pl.when((p == 4) & (v == 8))
            def _():
                diag_arrive(0)
        total = gate + 2 + 5 * at_2 + 3 * some + at_4

        def after(v, ls, c):
            @pl.when((p == 4) & ((v < 4) | (v == total - 1)))
            def _():
                publish(1, p1, r1, ls, c)
        partial_loop([
            (5 * at_0, near, ja, mine_w, 1),
            (4 * at_4, near, ob, mine_w + place(0), way),
            (1, near, ja, x_c, 1),
            (1, near, jb, y_c, 1),
            (5 * at_2, near, oa, mine_w, 1),
            (some, near, oa, other_w + first, way),
            (some, far, ja, mine_w + first, way),
            (some, far, ja, other_w + first, way),
            (at_4, near, ob, mine_w + place(4), 1),
        ], total, gate == 0, arrive_fn, before, after)
    for_each(NW, arrive)

    def d_copy(base, v, slot):
        return pltpu.make_async_copy(
            r0.at[pl.ds(mo((1 - j) * half, half), half), cols(base + v, 2)],
            bbuf.at[slot, pl.ds(0, half), :], bsem.at[slot])

    def b_copy(r, c, slot):
        return pltpu.make_async_copy(r.at[:, cols(c, 2)], bbuf.at[slot], bsem.at[slot])

    def on(v, values, body):
        hit = v == values[0]
        for value in values[1:]:
            hit = hit | (v == value)

        @pl.when(hit)
        def _():
            body()

    def pieces(q):
        d = diag_column(q)
        return [(1, near, jb, d, 1), (1, near, ob, d, 1), (1, far, jb, d, 1)]
    diag_unit = unit_table(
        [(NW, far, jb, mine_w, 1)] + pieces(0) + pieces(1) + [(NW, far, oa, mine_w, 1)]
        + pieces(2) + pieces(3) + [(NW, far, ob, mine_w, 1)] + pieces(4))
    pairs = 15

    def pair_copy(units, g, slot):
        return pltpu.make_async_copy(
            r0.at[inner(units[g][1]), cols(units[g][2], 2)],
            bbuf.at[slot, pl.ds(g * slab, slab), :], psem.at[slot, g])

    def before_diag(b):
        for q, arrival, reading in ((0, None, 2), (1, 3, 4), (2, 6, 8), (3, 9, None), (4, 12, 13)):
            if arrival is not None:
                on(b, (arrival,), lambda: diag_arrive(q))
            if reading is not None:
                on(b, (reading,), lambda: settle(0, p0, r0, 1 - l, diag_column(q)))

        @pl.when(b == pairs)
        def _():
            for ls in (0, 1):
                settle(1, p1, r1, ls, mine_w)
            b_copy(r1, mine_w, 1).start()

    def pair_at(b):
        return [diag_unit(2 * b), diag_unit(2 * b + 1)]

    first_pair = pair_at(jnp.int32(0))
    for g in (0, 1):
        pair_copy(first_pair, g, 0).start()

    def pair_step(b, carry):
        slot = lax.rem(b, 2)
        units = [carry[:3], carry[3:]]
        following = pair_at(b + 1)
        before_diag(b + 1)

        @pl.when(b + 1 < pairs)
        def _():
            pair_copy(following, 0, 1 - slot).start()

        @pl.when((b + 1 < pairs) & (b + 1 != 9))
        def _():
            pair_copy(following, 1, 1 - slot).start()
        for g in (0, 1):
            pair_copy(units, g, slot).wait()
        for g, (ls, ks, c) in enumerate(units):
            acc = jnp.dot(p0[rows(ls), inner(ks)], bbuf[slot, pl.ds(g * slab, slab), :],
                          preferred_element_type=jnp.float32)
            acc = acc + p1[rows(ls), cols(c, 2)].astype(jnp.float32)
            p1[rows(ls), cols(c, 2)] = jnp.minimum(acc, 1.0).astype(jnp.bfloat16)
        @pl.when(b + 1 == 9)
        def _():
            settle(0, p0, r0, 1 - l, diag_column(3))
            pair_copy(following, 1, 1 - slot).start()
        on(b, (3, 10, 11, 12, 13, 14), lambda: publish(1, p1, r1, units[0][0], units[0][2]))
        on(b, (4, 8, 11, 12), lambda: publish(1, p1, r1, units[1][0], units[1][2]))
        return (*following[0], *following[1])
    lax.fori_loop(0, pairs, pair_step, (*first_pair[0], *first_pair[1]))

    partner_sent(0, p0, 4 * NW)
    sent(x_copy, 0, p0, 3 * NW)
    sent(y_copy, 0, p0, 3 * NW)
    ready(0)

    def deep_loop(base, after, tail):
        span = pl.ds(mo((1 - j) * half, half), half)

        def step(v):
            slot = lax.rem(v, 2)

            @pl.when(v + 1 < NW)
            def _():
                d_copy(base, v + 1, 1 - slot).start()

            @pl.when(v + 1 == NW)
            def _():
                tail()
            d_copy(base, v, slot).wait()
            c = base + v
            acc = jnp.dot(p0[rows(1 - l), span], bbuf[slot, pl.ds(0, half), :], preferred_element_type=jnp.float32)
            acc = acc + p1[rows(1 - l), cols(c, 2)].astype(jnp.float32)
            p1[rows(1 - l), cols(c, 2)] = jnp.minimum(acc, 1.0).astype(jnp.bfloat16)
            after(c)
        for_each(NW, step)

    def unit_loop(start, stop, shift, where, r, src, dst, before, after, tail):
        def body(u):
            slot = lax.rem(u + shift, 2)
            ls, c = where(u)

            @pl.when(u + 1 < stop)
            def _():
                before(u + 1)
                b_copy(r, where(u + 1)[1], 1 - slot).start()

            @pl.when(u + 1 == stop)
            def _():
                tail()
            b_copy(r, c, slot).wait()
            acc = jnp.dot(src[rows(ls), :], bbuf[slot], preferred_element_type=jnp.float32)
            old = src[rows(ls), cols(c, 2)].astype(jnp.float32)
            dst[rows(ls), cols(c, 2)] = jnp.minimum(acc + old, 1.0).astype(jnp.bfloat16)
            after(u, ls, c)
        for_each(stop, body, start=start)

    def pick(u, table):
        found = table[-1]
        for index, value in enumerate(table[:-1]):
            found = jnp.where(u == index, value, found)
        return found

    def where2(u):
        own_u, diag_u, near_u = u < NW, u < 2 * NW, u < 3 * NW - X2
        ls = jnp.where(own_u | (~diag_u & near_u), l, 1 - l)
        c = jnp.where(own_u, mine_w + u, jnp.where(diag_u, other_w + u - NW, jnp.where(
            near_u, other_w + X2 + u - 2 * NW, mine_w + Y2 + u - 3 * NW + X2)))
        return ls, c

    def before2(u):
        @pl.when(u < 2 * NW)
        def _():
            for ls in (0, 1):
                settle(1, p1, r1, ls, where2(u)[1])

    def receive2_x(q):
        x_copy(1, pv(p0, l, mine_w, 2), pv(p0, l, other_w + q, 2), q).wait_recv()
        publish(2, p0, r2, l, other_w + q)

    def receive2_y(q):
        y_copy(1, pv(p0, l, mine_w, 2), pv(p0, 1 - l, mine_w + q, 2), q).wait_recv()
        publish(2, p0, r2, 1 - l, mine_w + q)

    def after2(u, ls, c):
        publish(2, p0, r2, ls, c)

        @pl.when(u == 0)
        def _():
            pl.semaphore_wait(rdy.at[0], 2)

        for copy, share in ((x_copy, X2), (y_copy, Y2)):
            @pl.when(u < share)
            def _():
                copy(1, pv(p0, l, mine_w + u, 2), pv(p0, l, mine_w + u, 2), u).start()

        for q, when in enumerate((5, 7, 11)):
            @pl.when(u == when)
            def _():
                receive2_x(q)
                receive2_y(q)

    def where3(u):
        own_u, near_u = u < NW, u < 2 * NW - X3
        ls = jnp.where(near_u, l, 1 - l)
        c = jnp.where(own_u, mine_w + pick(u, OWN3), jnp.where(
            near_u, other_w + X3 + u - NW, mine_w + Y3 + 1 + u - 2 * NW + X3))
        return ls, c

    def before3(u):
        @pl.when(u < 2 * NW - X3)
        def _():
            for ls in (0, 1):
                settle(2, p0, r2, ls, where3(u)[1])

    hrows = slab // 2

    def half_of(buf, base, ls, h):
        return buf.at[pl.ds(mo(base + ls * slab + h * hrows, hrows), hrows), cols(mine_w + Y3, 2)]

    def partner_half(src, h):
        return remote(src, half_of(r3, i * half, 1 - l, h), ps.at[3], pr.at[3, (1 - l) * 2 * NW + mine_w + Y3], p_dev)

    def local_half():
        return pltpu.make_async_copy(
            half_of(p1, 0, 1 - l, 1), half_of(r3, i * half, 1 - l, 1), loc.at[3, (1 - l) * 2 * NW + mine_w + Y3])

    def y_half(ls):
        return y_copy(2, half_of(p1, 0, l, 0), half_of(r3, i * half, ls, 0), Y3)

    def receive3(q):
        landed = rv(r3, 1 - l, mine_w + q, 2)
        y_copy(2, pv(p1, l, mine_w, 2), landed, q).wait_recv()
        partner_copy(3, landed, r3, 1 - l, mine_w + q).start()

    def receive3_half():
        y_half(1 - l).wait_recv()
        partner_half(half_of(r3, i * half, 1 - l, 0), 0).start()

    def half_unit(slot, tail):
        tail()
        b_copy(r2, mine_w + Y3, slot).wait()
        rs, cs = pl.ds(mo((1 - l) * slab + hrows, hrows), hrows), cols(mine_w + Y3, 2)
        acc = jnp.dot(p0[rs, :], bbuf[slot], preferred_element_type=jnp.float32)
        p1[rs, cs] = jnp.minimum(acc + p0[rs, cs].astype(jnp.float32), 1.0).astype(jnp.bfloat16)
        local_half().start()
        partner_half(half_of(p1, 0, 1 - l, 1), 1).start()

    def after3(u, ls, c):
        @pl.when((u < NW) | (u >= 2 * NW - X3))
        def _():
            publish(3, p1, r3, ls, c)

        @pl.when(u == 0)
        def _():
            pl.semaphore_wait(rdy.at[1], 2)

        @pl.when(u < X3)
        def _():
            x_copy(2, pv(p1, l, mine_w + u, 2), pv(p1, l, mine_w + u, 2), u).start()

        @pl.when(u < Y3)
        def _():
            y_copy(2, pv(p1, l, mine_w + u, 2), rv(r3, l, mine_w + u, 2), u).start()

        @pl.when(u == Y3)
        def _():
            y_half(l).start()

        @pl.when(u == 1)
        def _():
            receive2_y(3)

        @pl.when(u == 6)
        def _():
            receive3(0)

    def where4(u):
        return l, mine_w + pick(u, OWN4)

    def before4(u):
        c = where4(u)[1]
        settle(3, p1, r3, l, c)
        partner_copy(3, pv(p1, 1 - l, c, 2), r3, 1 - l, c).wait_recv()

        @pl.when(c == mine_w + Y3)
        def _():
            local_half().wait()

        @pl.when(c > mine_w + Y3)
        def _():
            local_copy(3, p1, r3, 1 - l, c).wait()

    def out_copy(u):
        c = where4(u)[1]
        return pltpu.make_async_copy(pv(p0, l, c, 2), o_ref.at[:, cols(c - mine_w, 2)], osem.at[0])

    def after4(u, ls, c):
        @pl.when(u == 1)
        def _():
            receive3_half()

        @pl.when(u > 0)
        def _():
            out_copy(u - 1).wait()
        out_copy(u).start()

    def read(r, where, before, u, slot):
        def start():
            before(jnp.int32(u))
            b_copy(r, where(jnp.int32(u))[1], slot).start()
        return start

    def no_tail():
        pass

    end2, end3 = 4 * NW - X2 - Y2, 3 * NW - X3 - Y3 - 1
    unit_loop(0, NW, 1, where2, r1, p1, p0, before2, after2, lambda: d_copy(other_w, 0, 0).start())
    deep_loop(other_w, lambda c: publish(1, p1, r1, 1 - l, c), read(r1, where2, before2, NW, 1))
    unit_loop(NW, end2, 0, where2, r1, p1, p0, before2, after2, read(r2, where3, before3, 0, end2 % 2))
    partner_sent(1, p1, 4 * NW)
    ready(1)
    shift3 = end2 % 2
    slot3 = (end3 + shift3) % 2
    unit_loop(0, end3, shift3, where3, r2, p0, p1, before3, after3, lambda: b_copy(r2, mine_w + Y3, slot3).start())
    half_unit(slot3, read(r3, where4, before4, 0, 1 - slot3))
    receive3(1)
    for_each(X3, lambda q: x_copy(2, pv(p1, l, mine_w, 2), pv(p1, l, other_w + q, 2), q).wait_recv())
    partner_sent(2, p0, 4 * NW)
    sent(x_copy, 1, p0, 2 * X2)
    sent(y_copy, 1, p0, 2 * Y2)

    def unused2(q):
        settle(2, p0, r2, 0, other_w + q)
        settle(2, p0, r2, 1, other_w + q)
    for_each(X3, unused2)
    unit_loop(0, NW, 1 - slot3, where4, r3, p1, p0, before4, after4, no_tail)
    partner_sent(3, p1, 2 * NW)
    sent(x_copy, 2, p1, 2 * X3)
    sent(y_copy, 2, p1, 2 * Y3 + 1)
    out_copy(NW - 1).wait()


def solution(mesh):
    layout = P(('row', 'depth'), 'col')

    def step(block):
        slab, half = block.shape
        n = 2 * half
        dma = pltpu.SemaphoreType.DMA
        whole = jax.ShapeDtypeStruct((n, n), block.dtype)
        hbm = pl.BlockSpec(memory_space=pltpu.HBM)
        return pl.pallas_call(
            functools.partial(kernel, n),
            out_shape=(jax.ShapeDtypeStruct(block.shape, block.dtype),) + (whole,) * 4,
            in_specs=[hbm],
            out_specs=(hbm,) * 5,
            scratch_shapes=[
                pltpu.VMEM((half, n), block.dtype),
                pltpu.VMEM((half, n), block.dtype),
                pltpu.VMEM((2, n, n // (2 * NW)), block.dtype),
                dma((4, 4 * NW)), dma((4,)), dma((4, 4 * NW)),
                dma((3,)), dma((NC + 2 * NW,)), dma((3,)), dma((NC + 2 * NW,)),
                dma((2,)), dma((2, 2)), dma((1,)), pltpu.SemaphoreType.REGULAR((2,)),
            ],
            compiler_params=pltpu.CompilerParams(
                collective_id=0, has_side_effects=True, vmem_limit_bytes=67043328),
            name='squarings',
        )(block)[0]

    return jax.shard_map(step, mesh=mesh, in_specs=(layout,), out_specs=layout, check_vma=False)
```

```python
import functools

import jax
import jax.numpy as jnp
from jax import lax
from jax.experimental import pallas as pl
from jax.experimental.pallas import tpu as pltpu
from jax.sharding import PartitionSpec as P

MESH = pl.DeviceIdType.MESH
NC = 10
NW = 5
X2, Y2 = 3, 4
X3, Y3 = 2, 2
OWN3 = (0, 1, 2, 4, 3)
OWN4 = (0, 3, 4, 1, 2)


def kernel(n, s_ref, o_ref, r0, r1, r2, r3, p0, p1, bbuf,
           loc, ps, pr, xs, xr, ys, yr, bsem, psem, osem, rdy):
    half, slab, width = n // 2, n // 4, n // (2 * NC)
    l = lax.axis_index('depth')
    j = lax.axis_index('col')
    i = lax.axis_index('row')
    x_dev, y_dev, p_dev = {'col': 1 - j}, {'depth': 1 - l}, {'row': 1 - i}

    def mo(v, m):
        return pl.multiple_of(v, m)

    def rows(ls):
        return pl.ds(mo(ls * slab, slab), slab)

    def cols(c, w=1):
        return pl.ds(mo(c * w * width, w * width), w * width)

    def pv(buf, ls, c, w=1):
        return buf.at[rows(ls), cols(c, w)]

    def rv(r, ls, c, w=1):
        return r.at[pl.ds(mo(i * half + ls * slab, slab), slab), cols(c, w)]

    def remote(src, dst, ssem, rsem, dev):
        return pltpu.make_async_remote_copy(
            src_ref=src, dst_ref=dst, send_sem=ssem, recv_sem=rsem, device_id=dev, device_id_type=MESH)

    def local_copy(k, buf, r, ls, c):
        return pltpu.make_async_copy(pv(buf, ls, c, 2), rv(r, ls, c, 2), loc.at[k, ls * 2 * NW + c])

    def partner_copy(k, src, r, ls, c):
        return remote(src, rv(r, ls, c, 2), ps.at[k], pr.at[k, ls * 2 * NW + c], p_dev)

    def x_copy(k, src, dst, q):
        return remote(src, dst, xs.at[k], xr.at[(0, NC, NC + NW)[k] + q], x_dev)

    def y_copy(k, src, dst, q):
        return remote(src, dst, ys.at[k], yr.at[(0, NC, NC + NW)[k] + q], y_dev)

    def publish(k, buf, r, ls, c):
        local_copy(k, buf, r, ls, c).start()
        partner_copy(k, pv(buf, ls, c, 2), r, ls, c).start()

    def settle(k, buf, r, ls, c):
        local_copy(k, buf, r, ls, c).wait()
        partner_copy(k, pv(buf, ls, c, 2), r, ls, c).wait_recv()

    def partner_sent(k, buf, count):
        part = buf.at[:, pl.ds(0, count * width)]
        remote(part, part, ps.at[k], pr.at[k, 0], p_dev).wait_send()

    def sent(copy, k, buf, count):
        part = buf.at[rows(0), pl.ds(0, count * width)]
        copy(k, part, part, 0).wait_send()

    def ready(k):
        for dev in (x_dev, y_dev):
            pl.semaphore_signal(rdy.at[k], inc=1, device_id=dev, device_id_type=MESH)

    def for_each(count, body, start=0):
        def step(q, carry):
            body(q)
            return carry
        lax.fori_loop(start, count, step, 0)

    mine, other = j * NC, (1 - j) * NC
    mine_w, other_w = j * NW, (1 - j) * NW

    barrier = pltpu.get_barrier_semaphore()
    for dev in (x_dev, y_dev, p_dev):
        pl.semaphore_signal(barrier, inc=1, device_id=dev, device_id_type=MESH)
    pl.semaphore_wait(barrier, 3)

    def place(p):
        return jnp.where(l == 0, p, NW - 1 - p)

    def diag_order(q):
        return 2 if q == 1 else 1 if q == 0 else 0 if q == 2 else q

    def own(c, w=2):
        return s_ref.at[:, cols(c, w)]

    def start_own(p):
        near_c, far_c = place(p), NW - 1 - place(p)
        x_copy(0, own(near_c), pv(p0, l, mine_w + near_c, 2), p).start()
        y_copy(0, own(far_c), pv(p0, l, mine_w + far_c, 2), p).start()
        partner_copy(0, own(near_c), r0, l, mine_w + near_c).start()
    for_each(NW, start_own)
    own_load = pltpu.make_async_copy(s_ref, p0.at[rows(l), pl.ds(mo(j * half, half), half)], osem.at[0])
    own_load.start()

    strip = slab // 10

    def merge(ls, c, mode):
        def body(q):
            rs = pl.ds(mo(ls * slab + q * strip, strip), strip)
            if mode == 'clear':
                p1[rs, cols(c, 2)] = jnp.zeros((strip, 2 * width), jnp.bfloat16)
            elif mode == 'copy':
                p1[rs, cols(c, 2)] = p0[rs, cols(c, 2)]
            else:
                p1[rs, cols(c, 2)] = jnp.maximum(p0[rs, cols(c, 2)], p1[rs, cols(c, 2)])
        for_each(10, body)

    for_each(NW, lambda p: merge(1 - l, other_w + p, 'clear'))
    own_load.wait()
    for_each(NW, lambda p: local_copy(0, p0, r0, l, mine_w + p).start())
    for_each(NW, lambda p: merge(l, mine_w + p, 'copy'))
    for_each(NW, lambda p: settle(0, p0, r0, l, mine_w + p))

    def inner(ks):
        return pl.ds(mo(ks * slab, slab), slab)

    def q_copy(ks, c, slot):
        return pltpu.make_async_copy(r0.at[inner(ks), cols(c, 2)], bbuf.at[slot, pl.ds(0, slab), :], bsem.at[slot])

    def unit_table(segments):
        def where(v):
            found, start = None, 0
            for count, ls, ks, first, stride in segments:
                here = (ls, ks, first + (v - start) * stride)
                if found is None:
                    found = here
                else:
                    later = v >= start
                    found = tuple(jnp.where(later, new, old) for new, old in zip(here, found))
                start = start + count
            return found
        return where

    def partial_loop(segments, total, first_gated, arrive_fn, before, after=None):
        where = unit_table(segments)
        begin = where(jnp.int32(0))

        @pl.when(jnp.logical_not(first_gated))
        def _():
            q_copy(begin[1], begin[2], 0).start()
        arrive_fn()
        before(jnp.int32(0))

        @pl.when(first_gated)
        def _():
            q_copy(begin[1], begin[2], 0).start()

        def step(v, carry):
            ls, ks, c = carry
            slot = lax.rem(v, 2)
            following = where(v + 1)
            before(v + 1)

            @pl.when(v + 1 < total)
            def _():
                q_copy(following[1], following[2], 1 - slot).start()
            q_copy(ks, c, slot).wait()
            acc = jnp.dot(p0[rows(ls), inner(ks)], bbuf[slot, pl.ds(0, slab), :], preferred_element_type=jnp.float32)
            acc = acc + p1[rows(ls), cols(c, 2)].astype(jnp.float32)
            p1[rows(ls), cols(c, 2)] = jnp.minimum(acc, 1.0).astype(jnp.bfloat16)
            if after is not None:
                after(v, ls, c)
            return following
        lax.fori_loop(0, total, step, begin)

    def flag(condition):
        return condition.astype(jnp.int32)

    ja, jb, oa, ob = 2 * j + l, 2 * j + 1 - l, 2 * (1 - j) + l, 2 * (1 - j) + 1 - l
    near, far = l, 1 - l

    def relay(q):
        a = diag_order(q)
        x_c = place(a)
        y_c = NW - 1 - x_c
        x_src = p0.at[rows(1 - l), cols(2 * (mine_w + x_c))]
        y_src = p0.at[rows(l), cols(2 * (other_w + y_c) + 1)]
        x_copy(0, x_src, x_src, NW + q).start()
        y_copy(0, y_src, y_src, NW + q).start()

    def diag_column(q):
        a = jnp.where(q == 0, 1, jnp.where(q == 1, 2, jnp.where(q == 2, 0, q)))
        return other_w + place(a)

    def diag_arrive(q):
        d = diag_column(q)
        x_copy(0, own(0, 1), p0.at[rows(1 - l), cols(2 * d)], NW + q).wait_recv()
        y_copy(0, own(0, 1), p0.at[rows(1 - l), cols(2 * d + 1)], NW + q).wait_recv()
        publish(0, p0, r0, 1 - l, d)
        merge(1 - l, d, 'max')

    def pieces(q):
        d = diag_column(q)
        return [(1, near, jb, d, 1), (1, near, ob, d, 1), (1, far, jb, d, 1)]
    diag_unit = unit_table(
        [(NW, far, jb, mine_w, 1)] + pieces(0) + pieces(1) + [(NW, far, oa, mine_w, 1)]
        + pieces(2) + pieces(3) + [(NW, far, ob, mine_w, 1)] + pieces(4))
    pairs = 15

    def pair_copy(units, g, slot):
        return pltpu.make_async_copy(
            r0.at[inner(units[g][1]), cols(units[g][2], 2)],
            bbuf.at[slot, pl.ds(g * slab, slab), :], psem.at[slot, g])

    def pair_at(b):
        return [diag_unit(2 * b), diag_unit(2 * b + 1)]

    first_pair = pair_at(jnp.int32(0))

    def arrive(p):
        x_c, y_c = other_w + place(p), mine_w + place(p)

        def arrive_fn():
            x_copy(0, own(0), pv(p0, l, x_c, 2), p).wait_recv()
            publish(0, p0, r0, l, x_c)
            y_copy(0, own(0), pv(p0, 1 - l, y_c, 2), p).wait_recv()
            publish(0, p0, r0, 1 - l, y_c)

            @pl.when(p == 3)
            def _():
                relay(0)
                relay(1)

            @pl.when(p == 4)
            def _():
                relay(2)
                relay(3)
                relay(4)
            merge(l, x_c, 'copy')
            merge(1 - l, y_c, 'copy')

        at_0, at_2, at_4, from_3 = flag(p == 0), flag(p == 2), flag(p == 4), flag(p > 2)
        some, first, way = 3 * at_2 + from_3, place(p * from_3), 1 - 2 * l
        gate = 5 * at_0 + 4 * at_4

        def before(v):
            @pl.when(v == gate)
            def _():
                settle(0, p0, r0, l, x_c)
                settle(0, p0, r0, 1 - l, y_c)

            @pl.when((p == 4) & (v == 8))
            def _():
                diag_arrive(0)

            @pl.when((p == 4) & (v == 10))
            def _():
                for g in (0, 1):
                    pair_copy(first_pair, g, 0).start()
        total = gate + 2 + 5 * at_2 + 3 * some + at_4

        def after(v, ls, c):
            @pl.when((p == 4) & ((v < 4) | (v == total - 1)))
            def _():
                publish(1, p1, r1, ls, c)
        partial_loop([
            (5 * at_0, near, ja, mine_w, 1),
            (4 * at_4, near, ob, mine_w + place(0), way),
            (1, near, ja, x_c, 1),
            (1, near, jb, y_c, 1),
            (5 * at_2, near, oa, mine_w, 1),
            (some, near, oa, other_w + first, way),
            (some, far, ja, mine_w + first, way),
            (some, far, ja, other_w + first, way),
            (at_4, near, ob, mine_w + place(4), 1),
        ], total, gate == 0, arrive_fn, before, after)
    for_each(NW, arrive)

    def d_copy(base, v, slot):
        return pltpu.make_async_copy(
            r0.at[pl.ds(mo((1 - j) * half, half), half), cols(base + v, 2)],
            bbuf.at[slot, pl.ds(0, half), :], bsem.at[slot])

    def b_copy(r, c, slot):
        return pltpu.make_async_copy(r.at[:, cols(c, 2)], bbuf.at[slot], bsem.at[slot])

    def on(v, values, body):
        hit = v == values[0]
        for value in values[1:]:
            hit = hit | (v == value)

        @pl.when(hit)
        def _():
            body()

    def before_diag(b):
        for q, arrival, reading in ((0, None, 2), (1, 3, 4), (2, 6, 8), (3, 9, None), (4, 12, 13)):
            if arrival is not None:
                on(b, (arrival,), lambda: diag_arrive(q))
            if reading is not None:
                on(b, (reading,), lambda: settle(0, p0, r0, 1 - l, diag_column(q)))

        @pl.when(b == pairs)
        def _():
            for ls in (0, 1):
                settle(1, p1, r1, ls, mine_w)
            b_copy(r1, mine_w, 1).start()


    def pair_step(b, carry):
        slot = lax.rem(b, 2)
        units = [carry[:3], carry[3:]]
        following = pair_at(b + 1)
        before_diag(b + 1)

        @pl.when(b + 1 < pairs)
        def _():
            pair_copy(following, 0, 1 - slot).start()

        @pl.when((b + 1 < pairs) & (b + 1 != 9))
        def _():
            pair_copy(following, 1, 1 - slot).start()
        for g in (0, 1):
            pair_copy(units, g, slot).wait()
        for g, (ls, ks, c) in enumerate(units):
            acc = jnp.dot(p0[rows(ls), inner(ks)], bbuf[slot, pl.ds(g * slab, slab), :],
                          preferred_element_type=jnp.float32)
            acc = acc + p1[rows(ls), cols(c, 2)].astype(jnp.float32)
            p1[rows(ls), cols(c, 2)] = jnp.minimum(acc, 1.0).astype(jnp.bfloat16)
        @pl.when(b + 1 == 9)
        def _():
            settle(0, p0, r0, 1 - l, diag_column(3))
            pair_copy(following, 1, 1 - slot).start()
        on(b, (3, 10, 11, 12, 13, 14), lambda: publish(1, p1, r1, units[0][0], units[0][2]))
        on(b, (4, 8, 11, 12), lambda: publish(1, p1, r1, units[1][0], units[1][2]))
        return (*following[0], *following[1])
    lax.fori_loop(0, pairs, pair_step, (*first_pair[0], *first_pair[1]))

    partner_sent(0, p0, 4 * NW)
    sent(x_copy, 0, p0, 3 * NW)
    sent(y_copy, 0, p0, 3 * NW)
    ready(0)

    def deep_loop(base, after, tail):
        span = pl.ds(mo((1 - j) * half, half), half)

        def step(v):
            slot = lax.rem(v, 2)

            @pl.when(v + 1 < NW)
            def _():
                d_copy(base, v + 1, 1 - slot).start()

            @pl.when(v + 1 == NW)
            def _():
                tail()
            d_copy(base, v, slot).wait()
            c = base + v
            acc = jnp.dot(p0[rows(1 - l), span], bbuf[slot, pl.ds(0, half), :], preferred_element_type=jnp.float32)
            acc = acc + p1[rows(1 - l), cols(c, 2)].astype(jnp.float32)
            p1[rows(1 - l), cols(c, 2)] = jnp.minimum(acc, 1.0).astype(jnp.bfloat16)
            after(c)
        for_each(NW, step)

    def unit_loop(start, stop, shift, where, r, src, dst, before, after, tail):
        def body(u):
            slot = lax.rem(u + shift, 2)
            ls, c = where(u)

            @pl.when(u + 1 < stop)
            def _():
                before(u + 1)
                b_copy(r, where(u + 1)[1], 1 - slot).start()

            @pl.when(u + 1 == stop)
            def _():
                tail()
            b_copy(r, c, slot).wait()
            acc = jnp.dot(src[rows(ls), :], bbuf[slot], preferred_element_type=jnp.float32)
            old = src[rows(ls), cols(c, 2)].astype(jnp.float32)
            dst[rows(ls), cols(c, 2)] = jnp.minimum(acc + old, 1.0).astype(jnp.bfloat16)
            after(u, ls, c)
        for_each(stop, body, start=start)

    def pick(u, table):
        found = table[-1]
        for index, value in enumerate(table[:-1]):
            found = jnp.where(u == index, value, found)
        return found

    def where2(u):
        own_u, diag_u, near_u = u < NW, u < 2 * NW, u < 3 * NW - X2
        ls = jnp.where(own_u | (~diag_u & near_u), l, 1 - l)
        c = jnp.where(own_u, mine_w + u, jnp.where(diag_u, other_w + u - NW, jnp.where(
            near_u, other_w + X2 + u - 2 * NW, mine_w + Y2 + u - 3 * NW + X2)))
        return ls, c

    def before2(u):
        @pl.when(u < 2 * NW)
        def _():
            for ls in (0, 1):
                settle(1, p1, r1, ls, where2(u)[1])

    def receive2_x(q):
        x_copy(1, pv(p0, l, mine_w, 2), pv(p0, l, other_w + q, 2), q).wait_recv()
        publish(2, p0, r2, l, other_w + q)

    def receive2_y(q):
        y_copy(1, pv(p0, l, mine_w, 2), pv(p0, 1 - l, mine_w + q, 2), q).wait_recv()
        publish(2, p0, r2, 1 - l, mine_w + q)

    def after2(u, ls, c):
        publish(2, p0, r2, ls, c)

        @pl.when(u == 0)
        def _():
            pl.semaphore_wait(rdy.at[0], 2)

        for copy, share in ((x_copy, X2), (y_copy, Y2)):
            @pl.when(u < share)
            def _():
                copy(1, pv(p0, l, mine_w + u, 2), pv(p0, l, mine_w + u, 2), u).start()

        for q, when in enumerate((5, 7, 11)):
            @pl.when(u == when)
            def _():
                receive2_x(q)
                receive2_y(q)

    def where3(u):
        own_u, near_u = u < NW, u < 2 * NW - X3
        ls = jnp.where(near_u, l, 1 - l)
        c = jnp.where(own_u, mine_w + pick(u, OWN3), jnp.where(
            near_u, other_w + X3 + u - NW, mine_w + Y3 + 1 + u - 2 * NW + X3))
        return ls, c

    def before3(u):
        @pl.when(u < 2 * NW - X3)
        def _():
            for ls in (0, 1):
                settle(2, p0, r2, ls, where3(u)[1])

    hrows = slab // 2

    def half_of(buf, base, ls, h):
        return buf.at[pl.ds(mo(base + ls * slab + h * hrows, hrows), hrows), cols(mine_w + Y3, 2)]

    def partner_half(src, h):
        return remote(src, half_of(r3, i * half, 1 - l, h), ps.at[3], pr.at[3, (1 - l) * 2 * NW + mine_w + Y3], p_dev)

    def local_half():
        return pltpu.make_async_copy(
            half_of(p1, 0, 1 - l, 1), half_of(r3, i * half, 1 - l, 1), loc.at[3, (1 - l) * 2 * NW + mine_w + Y3])

    def y_half(ls):
        return y_copy(2, half_of(p1, 0, l, 0), half_of(r3, i * half, ls, 0), Y3)

    def receive3(q):
        landed = rv(r3, 1 - l, mine_w + q, 2)
        y_copy(2, pv(p1, l, mine_w, 2), landed, q).wait_recv()
        partner_copy(3, landed, r3, 1 - l, mine_w + q).start()

    def receive3_half():
        y_half(1 - l).wait_recv()
        partner_half(half_of(r3, i * half, 1 - l, 0), 0).start()

    def half_unit(slot, tail):
        tail()
        b_copy(r2, mine_w + Y3, slot).wait()
        rs, cs = pl.ds(mo((1 - l) * slab + hrows, hrows), hrows), cols(mine_w + Y3, 2)
        acc = jnp.dot(p0[rs, :], bbuf[slot], preferred_element_type=jnp.float32)
        p1[rs, cs] = jnp.minimum(acc + p0[rs, cs].astype(jnp.float32), 1.0).astype(jnp.bfloat16)
        local_half().start()
        partner_half(half_of(p1, 0, 1 - l, 1), 1).start()

    def after3(u, ls, c):
        @pl.when((u < NW) | (u >= 2 * NW - X3))
        def _():
            publish(3, p1, r3, ls, c)

        @pl.when(u == 0)
        def _():
            pl.semaphore_wait(rdy.at[1], 2)

        @pl.when(u < X3)
        def _():
            x_copy(2, pv(p1, l, mine_w + u, 2), pv(p1, l, mine_w + u, 2), u).start()

        @pl.when(u < Y3)
        def _():
            y_copy(2, pv(p1, l, mine_w + u, 2), rv(r3, l, mine_w + u, 2), u).start()

        @pl.when(u == Y3)
        def _():
            y_half(l).start()

        @pl.when(u == 1)
        def _():
            receive2_y(3)

        @pl.when(u == 6)
        def _():
            receive3(0)

    def where4(u):
        return l, mine_w + pick(u, OWN4)

    def before4(u):
        c = where4(u)[1]
        settle(3, p1, r3, l, c)
        partner_copy(3, pv(p1, 1 - l, c, 2), r3, 1 - l, c).wait_recv()

        @pl.when(c == mine_w + Y3)
        def _():
            local_half().wait()

        @pl.when(c > mine_w + Y3)
        def _():
            local_copy(3, p1, r3, 1 - l, c).wait()

    def out_copy(u):
        c = where4(u)[1]
        return pltpu.make_async_copy(pv(p0, l, c, 2), o_ref.at[:, cols(c - mine_w, 2)], osem.at[0])

    def after4(u, ls, c):
        @pl.when(u == 1)
        def _():
            receive3_half()

        @pl.when(u > 0)
        def _():
            out_copy(u - 1).wait()
        out_copy(u).start()

    def read(r, where, before, u, slot):
        def start():
            before(jnp.int32(u))
            b_copy(r, where(jnp.int32(u))[1], slot).start()
        return start

    def no_tail():
        pass

    end2, end3 = 4 * NW - X2 - Y2, 3 * NW - X3 - Y3 - 1
    unit_loop(0, NW, 1, where2, r1, p1, p0, before2, after2, lambda: d_copy(other_w, 0, 0).start())
    deep_loop(other_w, lambda c: publish(1, p1, r1, 1 - l, c), read(r1, where2, before2, NW, 1))
    unit_loop(NW, end2, 0, where2, r1, p1, p0, before2, after2, read(r2, where3, before3, 0, end2 % 2))
    partner_sent(1, p1, 4 * NW)
    ready(1)
    shift3 = end2 % 2
    slot3 = (end3 + shift3) % 2
    unit_loop(0, end3, shift3, where3, r2, p0, p1, before3, after3, lambda: b_copy(r2, mine_w + Y3, slot3).start())
    half_unit(slot3, read(r3, where4, before4, 0, 1 - slot3))
    receive3(1)
    for_each(X3, lambda q: x_copy(2, pv(p1, l, mine_w, 2), pv(p1, l, other_w + q, 2), q).wait_recv())
    partner_sent(2, p0, 4 * NW)
    sent(x_copy, 1, p0, 2 * X2)
    sent(y_copy, 1, p0, 2 * Y2)

    def unused2(q):
        settle(2, p0, r2, 0, other_w + q)
        settle(2, p0, r2, 1, other_w + q)
    for_each(X3, unused2)
    unit_loop(0, NW, 1 - slot3, where4, r3, p1, p0, before4, after4, no_tail)
    partner_sent(3, p1, 2 * NW)
    sent(x_copy, 2, p1, 2 * X3)
    sent(y_copy, 2, p1, 2 * Y3 + 1)
    out_copy(NW - 1).wait()


def solution(mesh):
    layout = P(('row', 'depth'), 'col')

    def step(block):
        slab, half = block.shape
        n = 2 * half
        dma = pltpu.SemaphoreType.DMA
        whole = jax.ShapeDtypeStruct((n, n), block.dtype)
        hbm = pl.BlockSpec(memory_space=pltpu.HBM)
        return pl.pallas_call(
            functools.partial(kernel, n),
            out_shape=(jax.ShapeDtypeStruct(block.shape, block.dtype),) + (whole,) * 4,
            in_specs=[hbm],
            out_specs=(hbm,) * 5,
            scratch_shapes=[
                pltpu.VMEM((half, n), block.dtype),
                pltpu.VMEM((half, n), block.dtype),
                pltpu.VMEM((2, n, n // (2 * NW)), block.dtype),
                dma((4, 4 * NW)), dma((4,)), dma((4, 4 * NW)),
                dma((3,)), dma((NC + 2 * NW,)), dma((3,)), dma((NC + 2 * NW,)),
                dma((2,)), dma((2, 2)), dma((1,)), pltpu.SemaphoreType.REGULAR((2,)),
            ],
            compiler_params=pltpu.CompilerParams(
                collective_id=0, has_side_effects=True, vmem_limit_bytes=67043328),
            name='squarings',
        )(block)[0]

    return jax.shard_map(step, mesh=mesh, in_specs=(layout,), out_specs=layout, check_vma=False)
```
